32 devices in a mesh: bank: 4 (over y, x), zero: 8 (over z, core).
Axes of the slice: x: 2, y: 2, z: 4, core: 2. Of those that a mesh axis runs over, the one named last changes fastest.
Arguments:
- train_gate: float32 [64, 2048, 1024], P('bank', 'zero'), may hold values from -0.1875 to 0.1875
- train_up: float32 [64, 2048, 1024], P('bank', 'zero'), may hold values from -0.1875 to 0.1875
- train_down: float32 [64, 1024, 2048], P('bank', None, 'zero'), may hold values from -0.25 to 0.25
- router_weight: float32 [2048, 64], P('zero', 'bank'), may hold values from -0.125 to 0.125
- router_gain: float32 [2048], P('zero'), may hold values from 0.25 to 1.75
Outputs:
- ready_gate: bfloat16 [64, 2048, 1024], P('bank', None, 'zero')
- ready_up: bfloat16 [64, 2048, 1024], P('bank', None, 'zero')
- ready_down: bfloat16 [64, 1024, 2048], P('bank', 'zero')
- scale_gate: float32 [64, 1024], P('bank', 'zero')
- scale_up: float32 [64, 1024], P('bank', 'zero')
- scale_down: float32 [64, 1024], P('bank', 'zero')
- serve_router: bfloat16 [2048, 64], replicated
The draws below stay inside these ranges and needn't reach their ends.
All inputs are finite; a program needn't handle non-finite values.
Results may differ from the reference program's by a relative error of at most 0.001.
Values may be sent and summed in bfloat16 or wider, within the bound.
A program may use at most 192 MiB of HBM per device.

```python
import jax
import jax.numpy as jnp
from jax import lax

EXPERTS = 64
D_MODEL = 2048
D_EXPERT = 1024


def spiked(result, rng, source, target, blocks, factor):
    owner, partner = [(jnp.arange(result.shape[axis_at]) // (result.shape[axis_at] // blocks)).reshape([-1 if axis == axis_at else 1 for axis in range(result.ndim)]) for axis_at in (source, target)]
    chosen = jax.random.permutation(rng, blocks)[partner]
    strong = (owner == chosen) | (owner == (partner + blocks // 2) % blocks)
    return jnp.where(strong, factor * result, result)


def level_of(rng, shape, shards, least, top_value):
    factor_of, own = 1.0, jax.random.fold_in(rng, 6)
    for axis_at, shards_of in shards:
        heights = jnp.exp(jax.random.uniform(jax.random.fold_in(own, axis_at), (shards_of,), jnp.float32, least / len(shards), top_value / len(shards)))
        factor_of = factor_of * jnp.repeat(heights, shape[axis_at] // shards_of).reshape([-1 if axis == axis_at else 1 for axis in range(len(shape))])
    return factor_of


def scatter_about(own_key, shape, spread, limit, split=(), dtype=jnp.bfloat16):
    array = spread * jax.random.normal(own_key, shape, jnp.float32)
    if split:
        array = array * level_of(own_key, shape, split, -0.22, 0.18)
    return jnp.clip(array, -limit, limit).astype(dtype)


def noise_with(stream_key, extent, scale, reach, split, heavy, kind=jnp.bfloat16):
    drawn = scale * jax.random.normal(stream_key, extent, jnp.float32)
    if split:
        drawn = drawn * level_of(stream_key, extent, split, -0.22, 0.18)
    return jnp.clip(spiked(drawn, jax.random.fold_in(stream_key, 3), *heavy), -reach, reach).astype(kind)


def setup_inputs(seed: int = 0) -> dict:
    streams_of = jax.random.split(jax.random.key(seed), 6)
    return {
        "train_gate": noise_with(streams_of[0], (EXPERTS, D_MODEL, D_EXPERT), D_MODEL ** -0.5, 0.1875, ((0, 4), (1, 8)), (1, 2, 8, 2.0), jnp.float32),
        "train_up": noise_with(streams_of[1], (EXPERTS, D_MODEL, D_EXPERT), D_MODEL ** -0.5, 0.1875, ((0, 4), (1, 8)), (1, 2, 8, 2.0), jnp.float32),
        "train_down": noise_with(streams_of[2], (EXPERTS, D_EXPERT, D_MODEL), D_EXPERT ** -0.5, 0.25, ((0, 4), (2, 8)), (2, 1, 8, 2.0), jnp.float32),
        "router_weight": scatter_about(streams_of[3], (D_MODEL, EXPERTS), D_MODEL ** -0.5, 0.125, ((0, 8), (1, 4)), jnp.float32),
        "router_gain": jnp.clip(1.0 + 0.15 * jax.random.normal(streams_of[4], (D_MODEL,), jnp.float32), 0.25, 1.75),
    }


def reference(train_gate, train_up, train_down, router_weight, router_gain):
    scale_gate = jnp.sqrt(lax.optimization_barrier(jnp.sum(train_gate * train_gate, axis=1)))
    ready_gate = (train_gate / jnp.expand_dims(scale_gate, 1)).astype(jnp.bfloat16)
    scale_up = jnp.sqrt(lax.optimization_barrier(jnp.sum(train_up * train_up, axis=1)))
    ready_up = (train_up / jnp.expand_dims(scale_up, 1)).astype(jnp.bfloat16)
    scale_down = jnp.sqrt(lax.optimization_barrier(jnp.sum(train_down * train_down, axis=2)))
    ready_down = (train_down / jnp.expand_dims(scale_down, 2)).astype(jnp.bfloat16)
    serve_router = (router_weight * router_gain[:, None]).astype(jnp.bfloat16)
    return (ready_gate, ready_up, ready_down, scale_gate, scale_up, scale_down, serve_router)
```

```python
import functools

import jax
import jax.numpy as jnp
from jax import lax
from jax.experimental import pallas as pl
from jax.experimental.pallas import tpu as pltpu
from jax.sharding import PartitionSpec as P

MESH = pl.DeviceIdType.MESH


def exchange(
    n, chunk, near,
    gate, up, down, scale_gate, scale_up, scale_down,
    out_gate, out_up, out_down,
    wide, tall, send_gate, send_up, send_down, load_sem, send_sem, recv_sem,
):
    me = lax.axis_index("zero")
    experts = gate.shape[0]
    outs = (out_gate, out_up, out_down)
    sends = (send_gate, send_up, send_down)

    def place(t, first, count):
        if t < 2:
            rows = gate.shape[1]
            return outs[t].at[pl.ds(first, count), pl.ds(me * rows, rows), :]
        cols = down.shape[2]
        return outs[t].at[pl.ds(first, count), :, pl.ds(pl.multiple_of(me * cols, cols), cols)]

    def send(t, to, first, count):
        pltpu.make_async_remote_copy(
            src_ref=sends[t].at[to, pl.ds(first, count)],
            dst_ref=place(t, first, count),
            send_sem=send_sem.at[t],
            recv_sem=recv_sem.at[t],
            device_id={"zero": to},
            device_id_type=MESH,
        ).start()

    def send_at(t, distance, first, count):
        @pl.when(me + distance < n)
        def _():
            send(t, me + distance, first, count)

        @pl.when(me - distance >= 0)
        def _():
            send(t, me - distance, first, count)

    for t, (source, scale, buffer) in enumerate(
        ((gate, scale_gate, wide), (up, scale_up, wide), (down, scale_down, tall))
    ):

        def load(e):
            slot = lax.rem(e, 2)
            return pltpu.make_async_copy(source.at[e], buffer.at[slot], load_sem.at[slot])

        load(0).start()

        def narrow(e):
            @pl.when(e + 1 < experts)
            def _():
                load(e + 1).start()

            load(e).wait()
            slot = lax.rem(e, 2)
            if t < 2:
                width = source.shape[2] // n
                for d in range(n):
                    part = slice(d * width, (d + 1) * width)
                    inverse = 1.0 / scale[e, :, part]
                    sends[t][d, e] = (buffer[slot, :, part] * inverse).astype(jnp.bfloat16)
            else:
                height = source.shape[1] // n
                for d in range(n):
                    part = slice(d * height, (d + 1) * height)
                    inverse = 1.0 / scale[e, :, part]
                    column = jnp.transpose(jnp.broadcast_to(inverse, (128, height)))[:, :1]
                    sends[t][d, e] = (buffer[slot, part, :] * column).astype(jnp.bfloat16)

        def group(g, _):
            first = g * chunk
            lax.fori_loop(0, chunk, lambda k, _: narrow(first + k), None)
            for distance in range(1, near + 1):
                send_at(t, distance, first, chunk)

        lax.fori_loop(0, experts // chunk, group, None)
        pltpu.make_async_copy(sends[t].at[me], place(t, 0, experts), recv_sem.at[t]).start()

    for distance in range(near + 1, n):
        for t in range(3):
            send_at(t, distance, 0, experts)

    for t in range(3):
        others = sends[t].at[pl.ds(0, n - 1)]
        pltpu.make_async_copy(others, others, send_sem.at[t]).wait()
        pltpu.make_async_copy(outs[t], outs[t], recv_sem.at[t]).wait()


def exchange_call(n, gate, up, down, scale_gate, scale_up, scale_down):
    experts, rows, columns = gate.shape
    _, tall, short = down.shape
    hbm = pl.BlockSpec(memory_space=pl.ANY)
    vmem = pl.BlockSpec(memory_space=pltpu.VMEM)
    chunk = 2 if experts % 2 == 0 else 1
    return pl.pallas_call(
        functools.partial(exchange, n, chunk, min(3, n - 1)),
        out_shape=(
            jax.ShapeDtypeStruct((experts, rows * n, columns // n), jnp.bfloat16),
            jax.ShapeDtypeStruct((experts, rows * n, columns // n), jnp.bfloat16),
            jax.ShapeDtypeStruct((experts, tall // n, short * n), jnp.bfloat16),
        ),
        in_specs=[hbm] * 3 + [vmem] * 3,
        out_specs=(hbm, hbm, hbm),
        scratch_shapes=[
            pltpu.VMEM((2, rows, columns), jnp.float32),
            pltpu.VMEM((2, tall, short), jnp.float32),
            pltpu.VMEM((n, experts, rows, columns // n), jnp.bfloat16),
            pltpu.VMEM((n, experts, rows, columns // n), jnp.bfloat16),
            pltpu.VMEM((n, experts, tall // n, short), jnp.bfloat16),
            pltpu.SemaphoreType.DMA((2,)),
            pltpu.SemaphoreType.DMA((3,)),
            pltpu.SemaphoreType.DMA((3,)),
        ],
        compiler_params=pltpu.CompilerParams(
            has_side_effects=True, vmem_limit_bytes=48 * 1024 * 1024
        ),
    )(gate, up, down, scale_gate, scale_up, scale_down)


def on_device(n, train_gate, train_up, train_down, router_weight, router_gain):
    total_gate, total_up, total_down = lax.psum(
        (
            jnp.sum(train_gate * train_gate, axis=1),
            jnp.sum(train_up * train_up, axis=1),
            jnp.sum(train_down * train_down, axis=2),
        ),
        "zero",
    )
    scale_gate = jnp.sqrt(total_gate)
    scale_up = jnp.sqrt(total_up)
    scale_down = jnp.sqrt(total_down)
    aligned = (
        train_gate.shape[2] % (128 * n) == 0
        and train_down.shape[1] % (128 * n) == 0
        and train_down.shape[2] % 128 == 0
        and train_gate.shape[1] % 16 == 0
    )
    if aligned:
        ready_gate, ready_up, ready_down = exchange_call(
            n,
            train_gate,
            train_up,
            train_down,
            *(s[:, None, :] for s in (scale_gate, scale_up, scale_down)),
        )
    else:
        narrow_gate, narrow_up, narrow_down = (
            (train_gate / jnp.expand_dims(scale_gate, 1)).astype(jnp.bfloat16),
            (train_up / jnp.expand_dims(scale_up, 1)).astype(jnp.bfloat16),
            (train_down / jnp.expand_dims(scale_down, 2)).astype(jnp.bfloat16),
        )
        ready_gate, ready_up = (
            lax.all_to_all(narrow_gate, "zero", split_axis=2, concat_axis=1, tiled=True),
            lax.all_to_all(narrow_up, "zero", split_axis=2, concat_axis=1, tiled=True),
        )
        ready_down = lax.all_to_all(narrow_down, "zero", split_axis=1, concat_axis=2, tiled=True)
    scale_gate = lax.dynamic_slice_in_dim(
        scale_gate, lax.axis_index("zero") * ready_gate.shape[2], ready_gate.shape[2], axis=1
    )
    scale_up = lax.dynamic_slice_in_dim(
        scale_up, lax.axis_index("zero") * ready_up.shape[2], ready_up.shape[2], axis=1
    )
    scale_down = lax.dynamic_slice_in_dim(
        scale_down, lax.axis_index("zero") * ready_down.shape[1], ready_down.shape[1], axis=1
    )
    part_router = (router_weight * router_gain[:, None]).astype(jnp.bfloat16)
    row_router = lax.all_gather(part_router, "zero", axis=0, tiled=True)
    serve_router = lax.all_gather(row_router, "bank", axis=1, tiled=True)
    return (ready_gate, ready_up, ready_down, scale_gate, scale_up, scale_down, serve_router)


def solution(mesh):
    return jax.shard_map(
        functools.partial(on_device, mesh.shape["zero"]),
        mesh=mesh,
        in_specs=(
            P("bank", "zero", None),
            P("bank", "zero", None),
            P("bank", None, "zero"),
            P("zero", "bank"),
            P("zero"),
        ),
        out_specs=(
            P("bank", None, "zero"),
            P("bank", None, "zero"),
            P("bank", "zero", None),
            P("bank", "zero"),
            P("bank", "zero"),
            P("bank", "zero"),
            P(),
        ),
        check_vma=False,
    )
```

```python
import functools

import jax
import jax.numpy as jnp
from jax import lax
from jax.experimental import pallas as pl
from jax.experimental.pallas import tpu as pltpu
from jax.sharding import PartitionSpec as P

MESH = pl.DeviceIdType.MESH


def plain(train_gate, train_up, train_down, router_weight, router_gain):
    total_gate, total_up, total_down = lax.psum(
        (
            jnp.sum(train_gate * train_gate, axis=1),
            jnp.sum(train_up * train_up, axis=1),
            jnp.sum(train_down * train_down, axis=2),
        ),
        "zero",
    )
    scale_gate = jnp.sqrt(total_gate)
    scale_up = jnp.sqrt(total_up)
    scale_down = jnp.sqrt(total_down)
    narrow_gate, narrow_up, narrow_down = (
        (train_gate / jnp.expand_dims(scale_gate, 1)).astype(jnp.bfloat16),
        (train_up / jnp.expand_dims(scale_up, 1)).astype(jnp.bfloat16),
        (train_down / jnp.expand_dims(scale_down, 2)).astype(jnp.bfloat16),
    )
    ready_gate, ready_up = (
        lax.all_to_all(narrow_gate, "zero", split_axis=2, concat_axis=1, tiled=True),
        lax.all_to_all(narrow_up, "zero", split_axis=2, concat_axis=1, tiled=True),
    )
    ready_down = lax.all_to_all(narrow_down, "zero", split_axis=1, concat_axis=2, tiled=True)
    scale_gate = lax.dynamic_slice_in_dim(
        scale_gate, lax.axis_index("zero") * ready_gate.shape[2], ready_gate.shape[2], axis=1
    )
    scale_up = lax.dynamic_slice_in_dim(
        scale_up, lax.axis_index("zero") * ready_up.shape[2], ready_up.shape[2], axis=1
    )
    scale_down = lax.dynamic_slice_in_dim(
        scale_down, lax.axis_index("zero") * ready_down.shape[1], ready_down.shape[1], axis=1
    )
    part_router = (router_weight * router_gain[:, None]).astype(jnp.bfloat16)
    row_router = lax.all_gather(part_router, "zero", axis=0, tiled=True)
    serve_router = lax.all_gather(row_router, "bank", axis=1, tiled=True)
    return (ready_gate, ready_up, ready_down, scale_gate, scale_up, scale_down, serve_router)


def exchange(
    n, banks, chunk, near, slots,
    gate, up, down, router, gain,
    out_gate, out_up, out_down, scale_gate, scale_up, scale_down, out_router,
    wide, tall, send_gate, send_up, send_down, part, got, scales, rows_router,
    load_sem, send_sem, recv_sem, sum_send, sum_recv, scale_send, scale_recv, router_send, router_recv,
):
    me = lax.axis_index("zero")
    bank = lax.axis_index("bank")
    experts = gate.shape[0]
    sources = (gate, up, down)
    buffers = (wide, wide, tall)
    outs = (out_gate, out_up, out_down)
    sends = (send_gate, send_up, send_down)
    width = part.shape[-1]

    def to_peers(copy):
        for distance in range(1, n):

            @pl.when(me + distance < n)
            def _():
                copy(me + distance).start()

            @pl.when(me - distance >= 0)
            def _():
                copy(me - distance).start()

    def wait_for(refs, *sems):
        for sem in sems:
            pltpu.make_async_copy(refs, refs, sem).wait()

    def place(t, first, count):
        if t < 2:
            rows = gate.shape[1]
            return outs[t].at[pl.ds(first, count), pl.ds(me * rows, rows), :]
        cols = down.shape[2]
        return outs[t].at[pl.ds(first, count), :, pl.ds(pl.multiple_of(me * cols, cols), cols)]

    def send(t, to, first, count):
        pltpu.make_async_remote_copy(
            src_ref=sends[t].at[to, pl.ds(first, count)],
            dst_ref=place(t, first, count),
            send_sem=send_sem.at[t],
            recv_sem=recv_sem.at[t],
            device_id={"zero": to},
            device_id_type=MESH,
        ).start()

    def send_at(t, distance, first, count):
        @pl.when(me + distance < n)
        def _():
            send(t, me + distance, first, count)

        @pl.when(me - distance >= 0)
        def _():
            send(t, me - distance, first, count)

    def load(t, e):
        slot = lax.rem(e, slots)
        return pltpu.make_async_copy(sources[t].at[e], buffers[t].at[slot], load_sem.at[slot])

    def open_loads(t):
        for e in range(min(slots - 1, experts)):
            load(t, e).start()

    def arrived(t, e):
        @pl.when(e + slots - 1 < experts)
        def _():
            load(t, e + slots - 1).start()

        load(t, e).wait()
        return lax.rem(e, slots)

    def sums(t):
        open_loads(t)

        def body(e, _):
            slot = arrived(t, e)
            for d in range(n):
                piece = slice(d * width, (d + 1) * width)
                if t < 2:
                    x = buffers[t][slot, :, piece]
                    part[t, d, e] = jnp.sum(x * x, axis=0, keepdims=True)
                else:
                    total = None
                    for c in range(0, down.shape[2], 128):
                        x = buffers[t][slot, piece, c : c + 128]
                        total = x * x if total is None else total + x * x
                    part[t, d, e] = jnp.sum(jnp.transpose(total), axis=0, keepdims=True)

        lax.fori_loop(0, experts, body, None)
        got[t, me] = part[t, me]
        to_peers(
            lambda to: pltpu.make_async_remote_copy(
                src_ref=part.at[t, to],
                dst_ref=got.at[t, me],
                send_sem=sum_send.at[t],
                recv_sem=sum_recv.at[t],
                device_id={"zero": to},
                device_id_type=MESH,
            )
        )

    def finish_scale(t):
        wait_for(got.at[t, pl.ds(0, n - 1)], sum_recv.at[t])
        total = got[t, 0]
        for d in range(1, n):
            total = total + got[t, d]
        scale = jnp.sqrt(total)
        (scale_gate, scale_up, scale_down)[t][...] = scale
        scales[t, me] = scale
        to_peers(
            lambda to: pltpu.make_async_remote_copy(
                src_ref=scales.at[t, me],
                dst_ref=scales.at[t, me],
                send_sem=scale_send.at[t],
                recv_sem=scale_recv.at[t],
                device_id={"zero": to},
                device_id_type=MESH,
            )
        )

    def bulk(t):
        open_loads(t)
        wait_for(scales.at[t, pl.ds(0, n - 1)], scale_recv.at[t])

        def narrow(e):
            slot = arrived(t, e)
            for d in range(n):
                piece = slice(d * width, (d + 1) * width)
                inverse = 1.0 / scales[t, d, e]
                if t < 2:
                    ready = buffers[t][slot, :, piece] * inverse
                else:
                    column = jnp.transpose(jnp.broadcast_to(inverse, (128, width)))[:, :1]
                    ready = buffers[t][slot, piece, :] * column
                sends[t][d, e] = ready.astype(jnp.bfloat16)

        def group(g, _):
            first = g * chunk
            lax.fori_loop(0, chunk, lambda k, _: narrow(first + k), None)
            for distance in range(1, near + 1):
                send_at(t, distance, first, chunk)

        lax.fori_loop(0, experts // chunk, group, None)
        pltpu.make_async_copy(sends[t].at[me], place(t, 0, experts), recv_sem.at[t]).start()

    height, depth = router.shape
    block = out_router.at[pl.ds(pl.multiple_of(bank * height, height), height)]
    spot = out_router.at[
        pl.ds(pl.multiple_of(bank * height, height), height),
        pl.ds(pl.multiple_of(me * depth, depth), depth),
    ]
    rows_router[...] = (router[...] * gain[...]).astype(jnp.bfloat16)

    sums(0)
    to_peers(
        lambda to: pltpu.make_async_remote_copy(
            src_ref=rows_router,
            dst_ref=spot,
            send_sem=router_send.at[0],
            recv_sem=router_recv.at[0],
            device_id={"zero": to},
            device_id_type=MESH,
        )
    )
    pltpu.make_async_copy(rows_router, spot, router_recv.at[0]).start()
    sums(1)
    finish_scale(0)
    sums(2)
    finish_scale(1)
    wait_for(block, router_recv.at[0])
    for step in range(1, banks):
        pltpu.make_async_remote_copy(
            src_ref=block,
            dst_ref=block,
            send_sem=router_send.at[1],
            recv_sem=router_recv.at[1],
            device_id={"bank": lax.rem(bank + step, banks)},
            device_id_type=MESH,
        ).start()
    finish_scale(2)
    for t in range(3):
        bulk(t)
    for distance in range(near + 1, n):
        for t in range(3):
            send_at(t, distance, 0, experts)

    for t in range(3):
        wait_for(part.at[t, pl.ds(0, n - 1)], sum_send.at[t])
        wait_for(scales.at[t, pl.ds(0, n - 1)], scale_send.at[t])
        wait_for(sends[t].at[pl.ds(0, n - 1)], send_sem.at[t])
        wait_for(outs[t], recv_sem.at[t])
    wait_for(out_router.at[pl.ds(0, height), pl.ds(0, (n - 1) * depth)], router_send.at[0])
    wait_for(out_router.at[pl.ds(0, (banks - 1) * height)], router_send.at[1], router_recv.at[1])


def exchange_call(n, banks, gate, up, down, router, gain):
    experts, rows, columns = gate.shape
    _, tall, short = down.shape
    width = columns // n
    height, depth = router.shape
    hbm = pl.BlockSpec(memory_space=pl.ANY)
    vmem = pl.BlockSpec(memory_space=pltpu.VMEM)
    chunk = 2 if experts % 2 == 0 else 1
    slots = min(8, experts)
    scale = jax.ShapeDtypeStruct((experts, 1, width), jnp.float32)
    return pl.pallas_call(
        functools.partial(exchange, n, banks, chunk, min(3, n - 1), slots),
        out_shape=(
            jax.ShapeDtypeStruct((experts, rows * n, width), jnp.bfloat16),
            jax.ShapeDtypeStruct((experts, rows * n, width), jnp.bfloat16),
            jax.ShapeDtypeStruct((experts, width, short * n), jnp.bfloat16),
            scale,
            scale,
            scale,
            jax.ShapeDtypeStruct((height * banks, depth * n), jnp.bfloat16),
        ),
        in_specs=[hbm] * 3 + [vmem] * 2,
        out_specs=(hbm, hbm, hbm, vmem, vmem, vmem, hbm),
        scratch_shapes=[
            pltpu.VMEM((slots, rows, columns), jnp.float32),
            pltpu.VMEM((slots, tall, short), jnp.float32),
            pltpu.VMEM((n, experts, rows, width), jnp.bfloat16),
            pltpu.VMEM((n, experts, rows, width), jnp.bfloat16),
            pltpu.VMEM((n, experts, width, short), jnp.bfloat16),
            pltpu.VMEM((3, n, experts, 1, width), jnp.float32),
            pltpu.VMEM((3, n, experts, 1, width), jnp.float32),
            pltpu.VMEM((3, n, experts, 1, width), jnp.float32),
            pltpu.VMEM((height, depth), jnp.bfloat16),
            pltpu.SemaphoreType.DMA((slots,)),
            pltpu.SemaphoreType.DMA((3,)),
            pltpu.SemaphoreType.DMA((3,)),
            pltpu.SemaphoreType.DMA((3,)),
            pltpu.SemaphoreType.DMA((3,)),
            pltpu.SemaphoreType.DMA((3,)),
            pltpu.SemaphoreType.DMA((3,)),
            pltpu.SemaphoreType.DMA((2,)),
            pltpu.SemaphoreType.DMA((2,)),
        ],
        compiler_params=pltpu.CompilerParams(
            has_side_effects=True, vmem_limit_bytes=56 * 1024 * 1024
        ),
    )(gate, up, down, router, gain)


def on_device(n, banks, train_gate, train_up, train_down, router_weight, router_gain):
    aligned = (
        n > 1
        and banks > 1
        and train_gate.shape[2] == train_down.shape[1]
        and train_gate.shape[2] == 128 * n
        and train_down.shape[2] % 128 == 0
        and train_gate.shape[1] % 16 == 0
        and router_weight.shape[1] % 16 == 0
        and router_weight.shape[0] % 128 == 0
    )
    if not aligned:
        return plain(train_gate, train_up, train_down, router_weight, router_gain)
    *ready, scale_gate, scale_up, scale_down, router = exchange_call(
        n, banks, train_gate, train_up, train_down, router_weight.T, router_gain[None, :]
    )
    scales = (s[:, 0, :] for s in (scale_gate, scale_up, scale_down))
    return (*ready, *scales, router.T)


def solution(mesh):
    return jax.shard_map(
        functools.partial(on_device, mesh.shape["zero"], mesh.shape["bank"]),
        mesh=mesh,
        in_specs=(
            P("bank", "zero", None),
            P("bank", "zero", None),
            P("bank", None, "zero"),
            P("zero", "bank"),
            P("zero"),
        ),
        out_specs=(
            P("bank", None, "zero"),
            P("bank", None, "zero"),
            P("bank", "zero", None),
            P("bank", "zero"),
            P("bank", "zero"),
            P("bank", "zero"),
            P(),
        ),
        check_vma=False,
    )
```
